32 devices in a mesh: ep: 32 (over z, y, x, core).
Axes of the slice: x: 2, y: 2, z: 4, core: 2. Of those that a mesh axis runs over, the one named last changes fastest.
Arguments:
- hidden: bfloat16 [2, 1024, 3584], P(None, 'ep'), may hold values from -6 to 6
- expert_ids: int32 [2, 1024, 8], P(None, 'ep'), may hold values from 0 to 31, all different within a row; in each aligned block of 32 rows (0 to 31, 32 to 63, ..., all dimensions but the last counted through in order) at most 9 rows name the same one
- gate_scores: float32 [2, 1024, 8], P(None, 'ep'), may hold values from 0.05 to 1
- w_gate: bfloat16 [32, 3584, 1024], P('ep'), may hold values from -0.09375 to 0.09375
- w_up: bfloat16 [32, 3584, 1024], P('ep'), may hold values from -0.09375 to 0.09375
- w_down: bfloat16 [32, 1024, 3584], P('ep'), may hold values from -0.1875 to 0.1875
Outputs:
- mixed: bfloat16 [2, 1024, 3584], P(None, 'ep')
- expert_load: float32 [32], P('ep')
The draws below stay inside these ranges and needn't reach their ends.
Inputs may be any that keep to these rules, and one draw needn't show every extreme that they name: `expert_ids`: among the 32 rows of one device in one micro-batch, no expert is named by more than 9 rows, a bound that some block reaches. Each row names 8 different experts.
All inputs are finite; a program needn't handle non-finite values.
Results may differ from the reference program's by a relative error of at most 0.004.
The reference program's roundings to bfloat16 on the way (of `hid` and `answer`) count: a program that leaves them out, or rounds other values in their place, can miss the bound.
Values may be sent and summed in bfloat16 or wider, within the bound.
A program may use at most 128 MiB of HBM per device.

```python
import math
import jax
import jax.numpy as jnp
import numpy as np
from jax import lax

D = 3584
FF = 1024
TOP = 8
MICRO = 2
TOK_MB = 32
EXPERTS = 32
TOKENS = 1024
CAP = 9
N_EP = 32


def levels(own_key, extent, split, least, largest):
    factor_of = 1.0
    for axis_at, shards_of in split:
        heights = jax.random.uniform(jax.random.fold_in(jax.random.fold_in(own_key, 6), axis_at), (shards_of,), jnp.float32, least / len(split), largest / len(split))
        factor_of = factor_of * jnp.repeat(jnp.exp(heights), extent[axis_at] // shards_of).reshape((-1,) + (1,) * (len(extent) - 1 - axis_at))
    return factor_of


def shared_out(key, own, number, rows, count, top, most, skew):
    order = jax.random.permutation(key, count)
    heavy_load, ordinary = load_shares(count, rows * top, most, skew, True), load_shares(count, rows * top, most, skew, False)
    places = jnp.arange(count)

    def named(lengths, turn):
        used = int((lengths > 0).sum())
        fixed = max(1, used // 4)
        moved = fixed + (places - fixed + turn * (used - fixed)) % max(1, count - fixed)
        return jnp.zeros((count,), jnp.int32).at[order[jnp.where(places < fixed, places, moved)]].set(jnp.asarray(lengths, jnp.int32))

    lengths = jnp.where(number % 4 == 0, named(heavy_load, number // 4), named(ordinary, number - number // 4 - 1))
    mixed = jax.random.permutation(jax.random.fold_in(own, 3), count)
    source_of, receiver = mixed[0:count // 2 * 2:2], mixed[1:count // 2 * 2:2]
    slack = jnp.minimum(lengths[source_of] - 1, most - lengths[receiver]) // 2
    slack = jnp.where((source_of == order[0]) | (receiver == order[0]) | (lengths[receiver] == 0), 0, jnp.maximum(slack, 0))
    moved = jax.random.randint(jax.random.fold_in(own, 4), (count // 2,), 0, 1 << 20) % (slack + 1)
    lengths = lengths.at[source_of].add(-moved).at[receiver].add(moved)
    members = jnp.searchsorted(jnp.cumsum(lengths), jnp.arange(rows * top), side="right").astype(jnp.int32)
    table = members.reshape(top, rows).T
    table = table[jax.random.permutation(jax.random.fold_in(own, 1), rows)]
    turn = jax.random.randint(jax.random.fold_in(own, 2), (rows, 1), 0, top)
    return jnp.take_along_axis(table, (jnp.arange(top)[None, :] + turn) % top, axis=1)


def load_shares(amount, total, limit, lean, full):
    loads = [(1 << 20) // math.isqrt(rank ** lean) + 1 for rank in range(1, amount + 1)]
    largest = limit if full else min(limit, max(-(-total // amount), total * loads[0] // sum(loads)))
    least = 1 if total - largest >= amount - 1 else 0
    holding, rest = [largest] + [least] * (amount - 1), total - largest - least * (amount - 1)
    while rest > 0:
        candidates = [i for i in range(1, amount) if holding[i] < largest] or [i for i in range(1, amount) if holding[i] < limit]
        mass, left = sum([loads[i] for i in candidates]), rest
        for i in candidates:
            extra = min(limit - holding[i], max(1, left * loads[i] // mass), rest)
            holding[i] = holding[i] + extra
            rest = rest - extra
    return np.array(holding)


def noise(stream_key, shape, deviation, bound, shards=(), kind=jnp.bfloat16):
    values = jax.random.normal(stream_key, shape, jnp.float32) * deviation
    if len(shards) > 0:
        values = levels(stream_key, shape, shards, -0.22, 0.18) * values
    return jnp.clip(values, min=-bound, max=bound).astype(kind)


def setup_inputs(seed: int = 0) -> dict:
    arg_keys = jax.random.split(jax.random.key(seed), 7)
    hidden = noise(arg_keys[0], (MICRO, TOKENS, D), 1.0, 6.0, ((1, 32),))
    expert_ids_keys = jax.random.split(jax.random.fold_in(arg_keys[1], 1), MICRO * TOKENS // TOK_MB)
    expert_ids_turns = jax.random.permutation(jax.random.fold_in(arg_keys[1], 3), MICRO * TOKENS // TOK_MB)
    expert_ids = jax.vmap(lambda own, number: shared_out(jax.random.fold_in(arg_keys[1], 2), own, number, TOK_MB, EXPERTS, TOP, CAP, 2))(expert_ids_keys, expert_ids_turns).reshape((MICRO, TOKENS, TOP))
    gate_scores = jnp.clip(jnp.exp(math.log(1.0) - 2.9957323 * jax.random.uniform(arg_keys[2], (MICRO, TOKENS, TOP), jnp.float32) ** levels(arg_keys[2], (MICRO, TOKENS, TOP), ((1, 32),), -0.2, 0.2)), 0.05, 1.0)
    w_gate = noise(arg_keys[3], (EXPERTS, D, FF), D ** -0.5, 0.09375, ((0, 32),))
    w_up = noise(arg_keys[4], (EXPERTS, D, FF), D ** -0.5, 0.09375, ((0, 32),))
    w_down = noise(arg_keys[5], (EXPERTS, FF, D), FF ** -0.5, 0.1875, ((0, 32),))
    return dict(hidden=hidden, expert_ids=expert_ids, gate_scores=gate_scores, w_gate=w_gate, w_up=w_up, w_down=w_down)


route_scale = 2.5


def reference(hidden, expert_ids, gate_scores, w_gate, w_up, w_down):
    weights = route_scale * gate_scores / jnp.sum(gate_scores, axis=-1, keepdims=True)
    grouped = expert_ids.reshape(MICRO, N_EP, TOK_MB * TOP)
    one_hot = (grouped[..., None] == jnp.arange(EXPERTS, dtype=jnp.int32)).astype(jnp.int32)
    earlier = jnp.cumsum(one_hot, axis=2) - one_hot
    slot_index = jnp.sum(earlier * one_hot, axis=-1).astype(jnp.int32)
    batch_axis = jnp.arange(MICRO, dtype=jnp.int32)[:, None, None]
    source_axis = jnp.arange(N_EP, dtype=jnp.int32)[None, :, None]
    owner = (jnp.arange(TOK_MB * TOP, dtype=jnp.int32) // TOP)[None, None, :]
    token_row = (owner + source_axis * TOK_MB + batch_axis * TOKENS).astype(jnp.int32)
    table = jnp.full((MICRO, EXPERTS, N_EP, CAP), MICRO * TOKENS, jnp.int32)
    table = table.at[batch_axis, grouped, source_axis, slot_index].set(token_row)
    shares = jnp.zeros((MICRO, EXPERTS, N_EP, CAP), jnp.float32)
    shares = shares.at[batch_axis, grouped, source_axis, slot_index].set(weights.reshape(MICRO, N_EP, TOK_MB * TOP))
    padded = jnp.concatenate([hidden.reshape(MICRO * TOKENS, D), jnp.zeros((1, D), jnp.bfloat16)], axis=0)

    def expert_step(total, expert):
        rows_index = table[:, expert].reshape(-1)
        gathered = padded[rows_index]
        gate = jnp.dot(gathered, w_gate[expert], preferred_element_type=jnp.float32)
        upper = jnp.dot(gathered, w_up[expert], preferred_element_type=jnp.float32)
        hid = (jax.nn.silu(gate) * upper).astype(jnp.bfloat16)
        answer = jnp.dot(hid, w_down[expert], preferred_element_type=jnp.float32).astype(jnp.bfloat16)
        scaled = shares[:, expert].reshape(-1)[:, None] * answer.astype(jnp.float32)
        return total.at[rows_index].add(scaled), None

    start = jnp.zeros((MICRO * TOKENS + 1, D), jnp.float32)
    total, unused = lax.scan(expert_step, start, jnp.arange(EXPERTS, dtype=jnp.int32))
    mixed = total[: MICRO * TOKENS].reshape(MICRO, TOKENS, D).astype(jnp.bfloat16)
    sums = jnp.zeros((EXPERTS,), jnp.float32).at[expert_ids.reshape(-1)].add(weights.reshape(-1))
    expert_load = sums * (EXPERTS / (route_scale * MICRO * TOKENS))
    return mixed, expert_load
```

```python
import functools

import jax
import jax.numpy as jnp
from jax import lax
from jax.experimental import pallas as pl
from jax.experimental.pallas import tpu as pltpu
from jax.sharding import PartitionSpec as P

route_scale = 2.5
PLANE = 8
MESH = pl.DeviceIdType.MESH


def gather_kernel(
    planes, x_ref, g_ref, local_sem, recv_sem, core_recv, up_sem, down_sem, x_sem, y_sem, core_sem
):
    me = lax.axis_index("ep")
    p = me // PLANE
    quad = (me % PLANE) // 2
    core = me % 2
    x_quad = quad + 1 - 2 * (quad % 2)
    y_quad = (quad + 2) % 4
    d_quad = 3 - quad

    def dev(at_plane, at_quad, at_core=core):
        return at_plane * PLANE + at_quad * 2 + at_core

    up, down = me + PLANE, me - PLANE
    x_dev, y_dev, c_dev = dev(p, x_quad), dev(p, y_quad), dev(p, quad, 1 - core)

    barrier = pltpu.get_barrier_semaphore()
    for other in (x_dev, y_dev, c_dev):
        pl.semaphore_signal(barrier, inc=1, device_id=(other,), device_id_type=MESH)

    @pl.when(p < planes - 1)
    def _():
        pl.semaphore_signal(barrier, inc=1, device_id=(up,), device_id_type=MESH)

    @pl.when(p > 0)
    def _():
        pl.semaphore_signal(barrier, inc=1, device_id=(down,), device_id_type=MESH)

    below = (p + planes - 1) // planes
    above = (2 * planes - 2 - p) // planes
    pl.semaphore_wait(barrier, 3 + below + above)

    local = pltpu.make_async_copy(x_ref, g_ref.at[me], local_sem)
    local.start()

    def half(at_plane, at_quad, m, send_sem, to, own=False):
        place = g_ref.at[dev(at_plane, at_quad), m]
        return pltpu.make_async_remote_copy(
            src_ref=x_ref.at[m] if own else place,
            dst_ref=place,
            send_sem=send_sem,
            recv_sem=recv_sem.at[at_plane, at_quad, m],
            device_id=(to,),
            device_id_type=MESH,
        )

    def to_up(at_plane, m, own=False):
        return half(at_plane, quad, m, up_sem.at[at_plane, m], up, own)

    def to_down(at_plane, m, own=False):
        return half(at_plane, quad, m, down_sem.at[at_plane, m], down, own)

    def to_x(at_plane, m, own=False):
        return half(at_plane, quad, m, x_sem.at[at_plane, m], x_dev, own)

    def to_y(at_plane, m, own=False):
        return half(at_plane, quad, m, y_sem.at[at_plane, m], y_dev, own)

    def on_y(at_plane):
        return half(at_plane, x_quad, 0, y_sem.at[at_plane, 2], y_dev)

    def on_x(at_plane):
        return half(at_plane, y_quad, 1, x_sem.at[at_plane, 2], x_dev)

    def arrived(at_plane, at_quad, m):
        half(at_plane, at_quad, m, x_sem.at[at_plane, 0], x_dev).wait_recv()

    def to_core(at_plane, at_quad, own=False):
        place = g_ref.at[dev(at_plane, at_quad)]
        return pltpu.make_async_remote_copy(
            src_ref=x_ref if own else place,
            dst_ref=place,
            send_sem=core_sem.at[at_plane, at_quad],
            recv_sem=core_recv.at[at_plane, at_quad],
            device_id=(c_dev,),
            device_id_type=MESH,
        )

    def core_arrived(at_plane, at_quad):
        place = g_ref.at[dev(at_plane, at_quad, 1 - core)]
        pltpu.make_async_remote_copy(
            src_ref=place,
            dst_ref=place,
            send_sem=core_sem.at[at_plane, at_quad],
            recv_sem=core_recv.at[at_plane, at_quad],
            device_id=(c_dev,),
            device_id_type=MESH,
        ).wait_recv()

    for m in range(2):

        @pl.when(p < planes - 1)
        def _():
            to_up(p, m, True).start()

        @pl.when(p > 0)
        def _():
            to_down(p, m, True).start()

        to_x(p, m, True).start()
        to_y(p, m, True).start()
    to_core(p, quad, True).start()

    for s in range(1, planes):

        @pl.when(p >= s)
        def _():
            for m in range(2):
                arrived(p - s, quad, m)

                @pl.when(p < planes - 1)
                def _():
                    to_up(p - s, m).start()

                to_x(p - s, m).start()
                to_y(p - s, m).start()
            to_core(p - s, quad).start()

        @pl.when(p + s < planes)
        def _():
            for m in range(2):
                arrived(p + s, quad, m)

                @pl.when(p > 0)
                def _():
                    to_down(p + s, m).start()

                to_x(p + s, m).start()
                to_y(p + s, m).start()
            to_core(p + s, quad).start()

    def each(body):
        body(p)
        for s in range(1, planes):
            pl.when(p >= s)(functools.partial(body, p - s))
            pl.when(p + s < planes)(functools.partial(body, p + s))

    def across(at):
        arrived(at, x_quad, 0)
        on_y(at).start()
        arrived(at, y_quad, 0)
        arrived(at, y_quad, 1)
        on_x(at).start()
        arrived(at, x_quad, 1)
        to_core(at, x_quad).start()
        to_core(at, y_quad).start()

    def diagonal(at):
        arrived(at, d_quad, 0)
        arrived(at, d_quad, 1)
        to_core(at, d_quad).start()

    each(across)
    each(diagonal)

    def finish(at):
        for at_quad in (quad, x_quad, y_quad, d_quad):
            core_arrived(at, at_quad)
            to_core(at, at_quad).wait_send()
        for m in range(2):
            to_x(at, m).wait_send()
            to_y(at, m).wait_send()
        on_x(at).wait_send()
        on_y(at).wait_send()

    each(finish)
    for s in range(planes):

        @pl.when((p >= s) & (p < planes - 1))
        def _():
            for m in range(2):
                to_up(p - s, m).wait_send()

        @pl.when((p + s < planes) & (p > 0))
        def _():
            for m in range(2):
                to_down(p + s, m).wait_send()

    local.wait()


def gather_all(x, devices):
    planes = devices // PLANE
    dma = pltpu.SemaphoreType.DMA
    return pl.pallas_call(
        functools.partial(gather_kernel, planes),
        out_shape=jax.ShapeDtypeStruct((devices,) + x.shape, x.dtype),
        in_specs=[pl.BlockSpec(memory_space=pltpu.VMEM)],
        out_specs=pl.BlockSpec(memory_space=pl.ANY),
        scratch_shapes=[
            dma,
            dma((planes, 4, 2)),
            dma((planes, 4)),
            dma((planes, 2)),
            dma((planes, 2)),
            dma((planes, 3)),
            dma((planes, 3)),
            dma((planes, 4)),
        ],
        compiler_params=pltpu.CompilerParams(collective_id=0, has_side_effects=True),
    )(x)


def parts_of(values, count):
    parts = []
    for _ in range(count):
        part = lax.reduce_precision(values, 8, 7)
        parts.append(part.astype(jnp.bfloat16))
        values = values - part
    return parts


def ranks(mask):
    rows = mask.shape[-1]
    earlier = (jnp.arange(rows)[:, None] < jnp.arange(rows)[None, :]).astype(jnp.bfloat16)
    found = jnp.einsum(
        "...r,rt->...t", mask.astype(jnp.bfloat16), earlier, preferred_element_type=jnp.float32
    )
    return found.astype(jnp.int32)


def shards(hidden, expert_ids, gate_scores, w_gate, w_up, w_down):
    devices = lax.axis_size("ep")
    planes = devices // PLANE
    me = lax.axis_index("ep")
    my_plane, my_place = me // PLANE, me % PLANE
    micro_count, tok_mb, model_width = hidden.shape
    chosen = expert_ids.shape[2]
    capacity = tok_mb * chosen // devices + 1
    weights = route_scale * gate_scores / jnp.sum(gate_scores, axis=-1, keepdims=True)

    extra = jnp.concatenate([expert_ids.astype(jnp.bfloat16)] + parts_of(weights, 3), axis=-1)
    extra = jnp.pad(extra, ((0, 0), (0, 0), (0, 128 - extra.shape[-1])))
    everyone = gather_all(jnp.concatenate([hidden, extra], axis=-1), devices)

    notes = everyone[..., model_width:].astype(jnp.float32)
    all_ids = notes[..., :chosen].astype(jnp.int32)
    all_weights = (
        notes[..., chosen : 2 * chosen]
        + notes[..., 2 * chosen : 3 * chosen]
        + notes[..., 3 * chosen : 4 * chosen]
    )
    named = all_ids == me
    expert_load = jnp.sum(jnp.where(named, all_weights, 0.0)).reshape(1) * (
        devices / (route_scale * micro_count * tok_mb * devices)
    )

    mask = jnp.any(named, axis=-1)
    slots = jnp.arange(capacity, dtype=jnp.int32)
    hit = mask[:, :, None, :] & (ranks(mask)[:, :, None, :] == slots[:, None])
    row_at = jnp.sum(jnp.where(hit, jnp.arange(tok_mb, dtype=jnp.int32), 0), axis=-1)
    block_at = jnp.arange(devices * micro_count, dtype=jnp.int32).reshape(devices, micro_count, 1)
    row_at = (row_at + block_at * tok_mb).reshape(planes, PLANE, micro_count * capacity)
    row_at = row_at.transpose(1, 0, 2).reshape(-1)

    table = everyone.reshape(devices * micro_count * tok_mb, -1)
    rows = jnp.take(table, row_at, axis=0, mode="clip")[:, :model_width]
    gate = jnp.dot(rows, w_gate[0], preferred_element_type=jnp.float32)
    upper = jnp.dot(rows, w_up[0], preferred_element_type=jnp.float32)
    hid = (jax.nn.silu(gate) * upper).astype(jnp.bfloat16)
    answer = jnp.dot(hid, w_down[0], preferred_element_type=jnp.float32).astype(jnp.bfloat16)

    in_plane = [[k * PLANE + i for i in range(PLANE)] for k in range(planes)]
    in_column = [[k * PLANE + i for k in range(planes)] for i in range(PLANE)]
    returned = lax.all_to_all(
        answer.reshape(PLANE, -1, model_width),
        "ep",
        split_axis=0,
        concat_axis=0,
        tiled=True,
        axis_index_groups=in_plane,
    ).reshape(-1, model_width)

    column = (planes, PLANE) + all_ids.shape[1:]
    ids = lax.dynamic_index_in_dim(all_ids.reshape(column), my_place, 1, keepdims=False)
    share = lax.dynamic_index_in_dim(all_weights.reshape(column), my_place, 1, keepdims=False)
    experts_here = my_plane * PLANE + jnp.arange(PLANE, dtype=jnp.int32)
    same = ids[:, :, None] == experts_here[:, None, None]
    here = jnp.any(same, axis=-1)
    weight_here = jnp.sum(jnp.where(same, share[:, :, None], 0.0), axis=-1)
    spots = here[..., None] & (ranks(here)[..., None] == slots)
    spread = jnp.where(spots, weight_here[..., None], 0.0)
    spread = spread.transpose(0, 1, 3, 2, 4).reshape(planes * micro_count, tok_mb, PLANE, 1, capacity)
    diag = jnp.eye(planes * micro_count, dtype=jnp.float32)[:, None, None, :, None]
    matrix = (spread * diag).reshape(planes * micro_count * tok_mb, -1)
    partial = sum(
        jnp.dot(part, returned, preferred_element_type=jnp.float32) for part in parts_of(matrix, 2)
    ).astype(jnp.bfloat16)
    swapped = lax.all_to_all(
        partial.reshape(planes, micro_count * tok_mb, model_width),
        "ep",
        split_axis=0,
        concat_axis=0,
        tiled=True,
        axis_index_groups=in_column,
    )
    mixed = jnp.sum(swapped.astype(jnp.float32), axis=0).astype(jnp.bfloat16)
    return (mixed.reshape(micro_count, tok_mb, model_width), expert_load)


def solution(mesh):
    placed = (
        P(None, "ep", None),
        P(None, "ep", None),
        P(None, "ep", None),
        P("ep", None, None),
        P("ep", None, None),
        P("ep", None, None),
    )
    return jax.shard_map(
        shards,
        mesh=mesh,
        in_specs=placed,
        out_specs=(P(None, "ep", None), P("ep")),
        check_vma=False,
    )
```

```python
import functools

import jax
import jax.numpy as jnp
from jax import lax
from jax.experimental import pallas as pl
from jax.experimental.pallas import tpu as pltpu
from jax.sharding import PartitionSpec as P

route_scale = 2.5
PLANE = 8
MESH = pl.DeviceIdType.MESH


def gather_kernel(
    planes, x_ref, g_ref, local_sem, recv_sem, core_recv, up_sem, down_sem, x_sem, y_sem, core_sem
):
    me = lax.axis_index("ep")
    p = me // PLANE
    quad = (me % PLANE) // 2
    core = me % 2
    x_quad = quad + 1 - 2 * (quad % 2)
    y_quad = (quad + 2) % 4
    d_quad = 3 - quad

    def dev(at_plane, at_quad, at_core=core):
        return at_plane * PLANE + at_quad * 2 + at_core

    up, down = me + PLANE, me - PLANE
    x_dev, y_dev, c_dev = dev(p, x_quad), dev(p, y_quad), dev(p, quad, 1 - core)

    barrier = pltpu.get_barrier_semaphore()
    for other in (x_dev, y_dev, c_dev):
        pl.semaphore_signal(barrier, inc=1, device_id=(other,), device_id_type=MESH)

    @pl.when(p < planes - 1)
    def _():
        pl.semaphore_signal(barrier, inc=1, device_id=(up,), device_id_type=MESH)

    @pl.when(p > 0)
    def _():
        pl.semaphore_signal(barrier, inc=1, device_id=(down,), device_id_type=MESH)

    below = (p + planes - 1) // planes
    above = (2 * planes - 2 - p) // planes
    pl.semaphore_wait(barrier, 3 + below + above)

    local = pltpu.make_async_copy(x_ref, g_ref.at[me], local_sem)
    local.start()

    def half(at_plane, at_quad, m, send_sem, to, own=False):
        place = g_ref.at[dev(at_plane, at_quad), m]
        return pltpu.make_async_remote_copy(
            src_ref=x_ref.at[m] if own else place,
            dst_ref=place,
            send_sem=send_sem,
            recv_sem=recv_sem.at[at_plane, at_quad, m],
            device_id=(to,),
            device_id_type=MESH,
        )

    def to_up(at_plane, m, own=False):
        return half(at_plane, quad, m, up_sem.at[at_plane, m], up, own)

    def to_down(at_plane, m, own=False):
        return half(at_plane, quad, m, down_sem.at[at_plane, m], down, own)

    def to_x(at_plane, m, own=False):
        return half(at_plane, quad, m, x_sem.at[at_plane, m], x_dev, own)

    def to_y(at_plane, m, own=False):
        return half(at_plane, quad, m, y_sem.at[at_plane, m], y_dev, own)

    def on_y(at_plane):
        return half(at_plane, x_quad, 0, y_sem.at[at_plane, 2], y_dev)

    def on_x(at_plane):
        return half(at_plane, y_quad, 1, x_sem.at[at_plane, 2], x_dev)

    def arrived(at_plane, at_quad, m):
        half(at_plane, at_quad, m, x_sem.at[at_plane, 0], x_dev).wait_recv()

    def to_core(at_plane, at_quad, own=False):
        place = g_ref.at[dev(at_plane, at_quad)]
        return pltpu.make_async_remote_copy(
            src_ref=x_ref if own else place,
            dst_ref=place,
            send_sem=core_sem.at[at_plane, at_quad],
            recv_sem=core_recv.at[at_plane, at_quad],
            device_id=(c_dev,),
            device_id_type=MESH,
        )

    def core_arrived(at_plane, at_quad):
        place = g_ref.at[dev(at_plane, at_quad, 1 - core)]
        pltpu.make_async_remote_copy(
            src_ref=place,
            dst_ref=place,
            send_sem=core_sem.at[at_plane, at_quad],
            recv_sem=core_recv.at[at_plane, at_quad],
            device_id=(c_dev,),
            device_id_type=MESH,
        ).wait_recv()

    for m in range(2):

        @pl.when(p < planes - 1)
        def _():
            to_up(p, m, True).start()

        @pl.when(p > 0)
        def _():
            to_down(p, m, True).start()

        to_x(p, m, True).start()
        to_y(p, m, True).start()
    to_core(p, quad, True).start()

    for s in range(1, planes):

        @pl.when(p >= s)
        def _():
            for m in range(2):
                arrived(p - s, quad, m)

                @pl.when(p < planes - 1)
                def _():
                    to_up(p - s, m).start()

                to_x(p - s, m).start()
                to_y(p - s, m).start()
            to_core(p - s, quad).start()

        @pl.when(p + s < planes)
        def _():
            for m in range(2):
                arrived(p + s, quad, m)

                @pl.when(p > 0)
                def _():
                    to_down(p + s, m).start()

                to_x(p + s, m).start()
                to_y(p + s, m).start()
            to_core(p + s, quad).start()

    def each(body):
        body(p)
        for s in range(1, planes):
            pl.when(p >= s)(functools.partial(body, p - s))
            pl.when(p + s < planes)(functools.partial(body, p + s))

    def across(at):
        arrived(at, x_quad, 0)
        on_y(at).start()
        arrived(at, y_quad, 0)
        arrived(at, y_quad, 1)
        on_x(at).start()
        arrived(at, x_quad, 1)
        to_core(at, x_quad).start()
        to_core(at, y_quad).start()

    def diagonal(at):
        arrived(at, d_quad, 0)
        arrived(at, d_quad, 1)
        to_core(at, d_quad).start()

    each(across)
    each(diagonal)

    def finish(at):
        for at_quad in (quad, x_quad, y_quad, d_quad):
            core_arrived(at, at_quad)
            to_core(at, at_quad).wait_send()
        for m in range(2):
            to_x(at, m).wait_send()
            to_y(at, m).wait_send()
        on_x(at).wait_send()
        on_y(at).wait_send()

    each(finish)
    for s in range(planes):

        @pl.when((p >= s) & (p < planes - 1))
        def _():
            for m in range(2):
                to_up(p - s, m).wait_send()

        @pl.when((p + s < planes) & (p > 0))
        def _():
            for m in range(2):
                to_down(p + s, m).wait_send()

    local.wait()


def gather_all(x, devices):
    planes = devices // PLANE
    dma = pltpu.SemaphoreType.DMA
    return pl.pallas_call(
        functools.partial(gather_kernel, planes),
        out_shape=jax.ShapeDtypeStruct((devices,) + x.shape, x.dtype),
        in_specs=[pl.BlockSpec(memory_space=pltpu.VMEM)],
        out_specs=pl.BlockSpec(memory_space=pl.ANY),
        scratch_shapes=[
            dma,
            dma((planes, 4, 2)),
            dma((planes, 4)),
            dma((planes, 2)),
            dma((planes, 2)),
            dma((planes, 3)),
            dma((planes, 3)),
            dma((planes, 4)),
        ],
        compiler_params=pltpu.CompilerParams(collective_id=0, has_side_effects=True),
    )(x)


def return_kernel(
    planes, hid_ref, down_ref, matrix_ref, out_ref, w_buf, answers, inbox, sums, column, w_sem, a_send, a_recv, s_send, s_recv
):
    me = lax.axis_index("ep")
    p = me // PLANE
    q = me % PLANE
    chunks, depth, width = w_buf.shape

    def load(c):
        place = pl.multiple_of(c * width, width)
        return pltpu.make_async_copy(
            down_ref.at[:, pl.ds(place, width)], w_buf.at[c], w_sem.at[c]
        )

    for c in range(chunks):
        load(c).start()

    barrier = pltpu.get_barrier_semaphore()
    for i in range(1, PLANE):
        other = p * PLANE + (q + i) % PLANE
        pl.semaphore_signal(barrier, inc=1, device_id=(other,), device_id_type=MESH)
    for i in range(1, planes):
        other = ((p + i) % planes) * PLANE + q
        pl.semaphore_signal(barrier, inc=1, device_id=(other,), device_id_type=MESH)
    pl.semaphore_wait(barrier, PLANE + planes - 2)

    def answer_copy(c, i):
        place = (q + i) % PLANE
        return pltpu.make_async_remote_copy(
            src_ref=answers.at[c, place],
            dst_ref=inbox.at[c, q],
            send_sem=a_send.at[c, i],
            recv_sem=a_recv.at[c, q],
            device_id=(p * PLANE + place,),
            device_id_type=MESH,
        )

    def answer_arrived(c, i):
        place = (q + i) % PLANE
        pltpu.make_async_remote_copy(
            src_ref=answers.at[c, place],
            dst_ref=inbox.at[c, place],
            send_sem=a_send.at[c, i],
            recv_sem=a_recv.at[c, place],
            device_id=(p * PLANE + place,),
            device_id_type=MESH,
        ).wait_recv()

    def sum_copy(c, i):
        place = (p + i) % planes
        return pltpu.make_async_remote_copy(
            src_ref=sums.at[c, place],
            dst_ref=column.at[c, p],
            send_sem=s_send.at[c, i],
            recv_sem=s_recv.at[c, p],
            device_id=(place * PLANE + q,),
            device_id_type=MESH,
        )

    def sum_arrived(c, i):
        place = (p + i) % planes
        pltpu.make_async_remote_copy(
            src_ref=sums.at[c, place],
            dst_ref=column.at[c, place],
            send_sem=s_send.at[c, i],
            recv_sem=s_recv.at[c, place],
            device_id=(place * PLANE + q,),
            device_id_type=MESH,
        ).wait_recv()

    def compute(c, carry):
        load(c).wait()
        found = jnp.dot(hid_ref[...], w_buf[c], preferred_element_type=jnp.float32)
        answers[c] = found.reshape(answers.shape[1:]).astype(jnp.bfloat16)
        for i in range(1, PLANE):
            answer_copy(c, i).start()
        inbox[c, q] = answers[c, q]
        return carry

    lax.fori_loop(0, chunks, compute, 0)

    def combine(c, carry):
        for i in range(1, PLANE):
            answer_arrived(c, i)
        total = jnp.zeros((matrix_ref.shape[2], width), jnp.float32)
        for k in range(PLANE):
            for half in range(2):
                total += jnp.dot(
                    matrix_ref[k, half], inbox[c, k], preferred_element_type=jnp.float32
                )
        sums[c] = total.reshape(sums.shape[1:]).astype(jnp.bfloat16)
        for i in range(1, planes):
            sum_copy(c, i).start()
        column[c, p] = sums[c, p]
        return carry

    lax.fori_loop(0, chunks, combine, 0)

    def gather_sums(c, carry):
        for i in range(1, planes):
            sum_arrived(c, i)
        total = column[c, 0].astype(jnp.float32)
        for k in range(1, planes):
            total += column[c, k].astype(jnp.float32)
        out_ref[c] = total.astype(jnp.bfloat16)
        return carry

    lax.fori_loop(0, chunks, gather_sums, 0)

    def finish(c, carry):
        for i in range(1, PLANE):
            answer_copy(c, i).wait_send()
        for i in range(1, planes):
            sum_copy(c, i).wait_send()
        return carry

    lax.fori_loop(0, chunks, finish, 0)


def return_all(hid, w_down, matrix, devices):
    planes = devices // PLANE
    depth, model_width = w_down.shape
    width = next(w for w in (512, 256, 128) if model_width % w == 0)
    chunks = model_width // width
    rows = hid.shape[0] // PLANE
    tokens = matrix.shape[2] // planes
    dma = pltpu.SemaphoreType.DMA
    vmem = pl.BlockSpec(memory_space=pltpu.VMEM)
    return pl.pallas_call(
        functools.partial(return_kernel, planes),
        out_shape=jax.ShapeDtypeStruct((chunks, tokens, width), jnp.bfloat16),
        in_specs=[vmem, pl.BlockSpec(memory_space=pl.ANY), vmem],
        out_specs=vmem,
        scratch_shapes=[
            pltpu.VMEM((chunks, depth, width), jnp.bfloat16),
            pltpu.VMEM((chunks, PLANE, rows, width), jnp.bfloat16),
            pltpu.VMEM((chunks, PLANE, rows, width), jnp.bfloat16),
            pltpu.VMEM((chunks, planes, tokens, width), jnp.bfloat16),
            pltpu.VMEM((chunks, planes, tokens, width), jnp.bfloat16),
            dma((chunks,)),
            dma((chunks, PLANE)),
            dma((chunks, PLANE)),
            dma((chunks, planes)),
            dma((chunks, planes)),
        ],
        compiler_params=pltpu.CompilerParams(collective_id=1, has_side_effects=True),
    )(hid, w_down, matrix)


def parts_of(values, count):
    parts = []
    for _ in range(count):
        part = lax.reduce_precision(values, 8, 7)
        parts.append(part.astype(jnp.bfloat16))
        values = values - part
    return parts


def ranks(mask):
    rows = mask.shape[-1]
    earlier = (jnp.arange(rows)[:, None] < jnp.arange(rows)[None, :]).astype(jnp.bfloat16)
    found = jnp.einsum(
        "...r,rt->...t", mask.astype(jnp.bfloat16), earlier, preferred_element_type=jnp.float32
    )
    return found.astype(jnp.int32)


def shards(hidden, expert_ids, gate_scores, w_gate, w_up, w_down):
    devices = lax.axis_size("ep")
    planes = devices // PLANE
    me = lax.axis_index("ep")
    my_plane, my_place = me // PLANE, me % PLANE
    micro_count, tok_mb, model_width = hidden.shape
    chosen = expert_ids.shape[2]
    capacity = tok_mb * chosen // devices + 1
    weights = route_scale * gate_scores / jnp.sum(gate_scores, axis=-1, keepdims=True)

    extra = jnp.concatenate([expert_ids.astype(jnp.bfloat16)] + parts_of(weights, 3), axis=-1)
    extra = jnp.pad(extra, ((0, 0), (0, 0), (0, 128 - extra.shape[-1])))
    everyone = gather_all(jnp.concatenate([hidden, extra], axis=-1), devices)

    notes = everyone[..., model_width:].astype(jnp.float32)
    all_ids = notes[..., :chosen].astype(jnp.int32)
    all_weights = (
        notes[..., chosen : 2 * chosen]
        + notes[..., 2 * chosen : 3 * chosen]
        + notes[..., 3 * chosen : 4 * chosen]
    )
    named = all_ids == me
    expert_load = jnp.sum(jnp.where(named, all_weights, 0.0)).reshape(1) * (
        devices / (route_scale * micro_count * tok_mb * devices)
    )

    mask = jnp.any(named, axis=-1)
    slots = jnp.arange(capacity, dtype=jnp.int32)
    hit = mask[:, :, None, :] & (ranks(mask)[:, :, None, :] == slots[:, None])
    row_at = jnp.sum(jnp.where(hit, jnp.arange(tok_mb, dtype=jnp.int32), 0), axis=-1)
    block_at = jnp.arange(devices * micro_count, dtype=jnp.int32).reshape(devices, micro_count, 1)
    row_at = (row_at + block_at * tok_mb).reshape(planes, PLANE, micro_count * capacity)
    row_at = row_at.transpose(1, 0, 2).reshape(-1)

    table = everyone.reshape(devices * micro_count * tok_mb, -1)
    rows = jnp.take(table, row_at, axis=0, mode="clip")[:, :model_width]
    gate = jnp.dot(rows, w_gate[0], preferred_element_type=jnp.float32)
    upper = jnp.dot(rows, w_up[0], preferred_element_type=jnp.float32)
    hid = (jax.nn.silu(gate) * upper).astype(jnp.bfloat16)

    column = (planes, PLANE) + all_ids.shape[1:]
    ids = lax.dynamic_index_in_dim(all_ids.reshape(column), my_place, 1, keepdims=False)
    share = lax.dynamic_index_in_dim(all_weights.reshape(column), my_place, 1, keepdims=False)
    experts_here = my_plane * PLANE + jnp.arange(PLANE, dtype=jnp.int32)
    same = ids[:, :, None] == experts_here[:, None, None]
    here = jnp.any(same, axis=-1)
    weight_here = jnp.sum(jnp.where(same, share[:, :, None], 0.0), axis=-1)
    spots = here[..., None] & (ranks(here)[..., None] == slots)
    spread = jnp.where(spots, weight_here[..., None], 0.0)
    groups = planes * micro_count
    spread = spread.transpose(2, 0, 1, 3, 4).reshape(PLANE, groups, tok_mb, 1, capacity)
    diag = jnp.eye(groups, dtype=jnp.float32)[:, None, :, None]
    matrix = (spread * diag).reshape(PLANE, groups * tok_mb, groups * capacity)
    matrix = jnp.stack(parts_of(matrix, 2), axis=1)
    mixed = return_all(hid, w_down[0], matrix, devices)
    mixed = mixed.transpose(1, 0, 2)
    return (mixed.reshape(micro_count, tok_mb, model_width), expert_load)


def solution(mesh):
    placed = (
        P(None, "ep", None),
        P(None, "ep", None),
        P(None, "ep", None),
        P("ep", None, None),
        P("ep", None, None),
        P("ep", None, None),
    )
    return jax.shard_map(
        shards,
        mesh=mesh,
        in_specs=placed,
        out_specs=(P(None, "ep", None), P("ep")),
        check_vma=False,
    )
```

```python
import functools

import jax
import jax.numpy as jnp
from jax import lax
from jax.experimental import pallas as pl
from jax.experimental.pallas import tpu as pltpu
from jax.sharding import PartitionSpec as P

route_scale = 2.5
PLANE = 8
MESH = pl.DeviceIdType.MESH


def gather_kernel(
    planes,
    capacity,
    chosen,
    x_ref,
    g_ref,
    rows_ref,
    notes_ref,
    table,
    local_sem,
    recv_sem,
    core_recv,
    up_sem,
    down_sem,
    x_sem,
    y_sem,
    core_sem,
    table_sem,
):
    me = lax.axis_index("ep")
    p = me // PLANE
    quad = (me % PLANE) // 2
    core = me % 2
    x_quad = quad + 1 - 2 * (quad % 2)
    y_quad = (quad + 2) % 4
    d_quad = 3 - quad

    def dev(at_plane, at_quad, at_core=core):
        return at_plane * PLANE + at_quad * 2 + at_core

    def block(at_plane, at_quad, at_core=core):
        return g_ref.at[at_quad * 2 + at_core, at_plane]

    up, down = me + PLANE, me - PLANE
    x_dev, y_dev, c_dev = dev(p, x_quad), dev(p, y_quad), dev(p, quad, 1 - core)

    barrier = pltpu.get_barrier_semaphore()
    for other in (x_dev, y_dev, c_dev):
        pl.semaphore_signal(barrier, inc=1, device_id=(other,), device_id_type=MESH)

    @pl.when(p < planes - 1)
    def _():
        pl.semaphore_signal(barrier, inc=1, device_id=(up,), device_id_type=MESH)

    @pl.when(p > 0)
    def _():
        pl.semaphore_signal(barrier, inc=1, device_id=(down,), device_id_type=MESH)

    below = (p + planes - 1) // planes
    above = (2 * planes - 2 - p) // planes
    pl.semaphore_wait(barrier, 3 + below + above)

    local = pltpu.make_async_copy(x_ref, block(p, quad), local_sem)
    local.start()

    def half(at_plane, at_quad, m, send_sem, to, own=False):
        place = block(at_plane, at_quad).at[m]
        return pltpu.make_async_remote_copy(
            src_ref=x_ref.at[m] if own else place,
            dst_ref=place,
            send_sem=send_sem,
            recv_sem=recv_sem.at[at_plane, at_quad, m],
            device_id=(to,),
            device_id_type=MESH,
        )

    def to_up(at_plane, m, own=False):
        return half(at_plane, quad, m, up_sem.at[at_plane, m], up, own)

    def to_down(at_plane, m, own=False):
        return half(at_plane, quad, m, down_sem.at[at_plane, m], down, own)

    def to_x(at_plane, m, own=False):
        return half(at_plane, quad, m, x_sem.at[at_plane, m], x_dev, own)

    def to_y(at_plane, m, own=False):
        return half(at_plane, quad, m, y_sem.at[at_plane, m], y_dev, own)

    def on_y(at_plane):
        return half(at_plane, x_quad, 0, y_sem.at[at_plane, 2], y_dev)

    def on_x(at_plane):
        return half(at_plane, y_quad, 1, x_sem.at[at_plane, 2], x_dev)

    def arrived(at_plane, at_quad, m):
        half(at_plane, at_quad, m, x_sem.at[at_plane, 0], x_dev).wait_recv()

    def to_core(at_plane, at_quad, own=False):
        place = block(at_plane, at_quad)
        return pltpu.make_async_remote_copy(
            src_ref=x_ref if own else place,
            dst_ref=place,
            send_sem=core_sem.at[at_plane, at_quad],
            recv_sem=core_recv.at[at_plane, at_quad],
            device_id=(c_dev,),
            device_id_type=MESH,
        )

    def core_arrived(at_plane, at_quad):
        place = block(at_plane, at_quad, 1 - core)
        pltpu.make_async_remote_copy(
            src_ref=place,
            dst_ref=place,
            send_sem=core_sem.at[at_plane, at_quad],
            recv_sem=core_recv.at[at_plane, at_quad],
            device_id=(c_dev,),
            device_id_type=MESH,
        ).wait_recv()

    for m in range(2):

        @pl.when(p < planes - 1)
        def _():
            to_up(p, m, True).start()

        @pl.when(p > 0)
        def _():
            to_down(p, m, True).start()

        to_x(p, m, True).start()
        to_y(p, m, True).start()
    to_core(p, quad, True).start()

    for s in range(1, planes):

        @pl.when(p >= s)
        def _():
            for m in range(2):
                arrived(p - s, quad, m)

                @pl.when(p < planes - 1)
                def _():
                    to_up(p - s, m).start()

                to_x(p - s, m).start()
                to_y(p - s, m).start()
            to_core(p - s, quad).start()

        @pl.when(p + s < planes)
        def _():
            for m in range(2):
                arrived(p + s, quad, m)

                @pl.when(p > 0)
                def _():
                    to_down(p + s, m).start()

                to_x(p + s, m).start()
                to_y(p + s, m).start()
            to_core(p + s, quad).start()

    def each(body):
        body(p)
        for s in range(1, planes):
            pl.when(p >= s)(functools.partial(body, p - s))
            pl.when(p + s < planes)(functools.partial(body, p + s))

    def across(at):
        arrived(at, x_quad, 0)
        on_y(at).start()
        arrived(at, y_quad, 0)
        arrived(at, y_quad, 1)
        on_x(at).start()
        arrived(at, x_quad, 1)
        to_core(at, x_quad).start()
        to_core(at, y_quad).start()

    def diagonal(at):
        arrived(at, d_quad, 0)
        arrived(at, d_quad, 1)
        to_core(at, d_quad).start()

    local.wait()

    tok_mb, wide = x_ref.shape[1:]
    depth = planes * 2 * tok_mb
    model_width = rows_ref.shape[2]
    token = lax.broadcasted_iota(jnp.int32, (depth, depth), 0)
    other = lax.broadcasted_iota(jnp.int32, (depth, depth), 1)
    before = (other < token) & (lax.div(other, tok_mb) == lax.div(token, tok_mb))
    before = jnp.where(before, 1.0, 0.0).astype(jnp.bfloat16)
    lanes = (depth, 128)
    start = lax.div(lax.broadcasted_iota(jnp.int32, lanes, 0), tok_mb) * capacity
    lane = lax.broadcasted_iota(jnp.int32, lanes, 1)

    def fetch(place, slot):
        return pltpu.make_async_copy(g_ref.at[place], table.at[slot], table_sem.at[slot])

    def select(place, slot):
        fetch(place, slot).wait()
        notes = table[slot, :, :, :, model_width:]
        notes_ref[place] = notes
        ids = notes.reshape(lanes).astype(jnp.float32).astype(jnp.int32)
        named = jnp.where((ids == me) & (lane < chosen), 1.0, 0.0)
        named = jnp.broadcast_to(jnp.sum(named, axis=1, keepdims=True), lanes)
        rank = jnp.dot(before, named.astype(jnp.bfloat16), preferred_element_type=jnp.float32)
        spot = start + rank.astype(jnp.int32)
        pick = jnp.where((lane == spot) & (named > 0.5), 1.0, 0.0).astype(jnp.bfloat16)
        found = lax.dot_general(
            pick,
            table[slot, :, :, :, :model_width].reshape(depth, model_width),
            (((0,), (0,)), ((), ())),
            preferred_element_type=jnp.float32,
        )
        rows_ref[place] = found[: rows_ref.shape[1]].astype(jnp.bfloat16)

    each(across)

    def others(at_quad):
        each(lambda at: core_arrived(at, at_quad))

    fetch(quad * 2 + core, 0).start()
    fetch(x_quad * 2 + core, 1).start()
    select(quad * 2 + core, 0)
    fetch(y_quad * 2 + core, 0).start()
    select(x_quad * 2 + core, 1)
    others(quad)
    fetch(quad * 2 + 1 - core, 1).start()
    select(y_quad * 2 + core, 0)
    others(x_quad)
    fetch(x_quad * 2 + 1 - core, 0).start()
    select(quad * 2 + 1 - core, 1)
    each(diagonal)
    fetch(d_quad * 2 + core, 1).start()
    select(x_quad * 2 + 1 - core, 0)
    others(y_quad)
    fetch(y_quad * 2 + 1 - core, 0).start()
    select(d_quad * 2 + core, 1)
    others(d_quad)
    fetch(d_quad * 2 + 1 - core, 1).start()
    select(y_quad * 2 + 1 - core, 0)
    select(d_quad * 2 + 1 - core, 1)

    def finish(at):
        for at_quad in (quad, x_quad, y_quad, d_quad):
            to_core(at, at_quad).wait_send()
        for m in range(2):
            to_x(at, m).wait_send()
            to_y(at, m).wait_send()
        on_x(at).wait_send()
        on_y(at).wait_send()

    each(finish)
    for s in range(planes):

        @pl.when((p >= s) & (p < planes - 1))
        def _():
            for m in range(2):
                to_up(p - s, m).wait_send()

        @pl.when((p + s < planes) & (p > 0))
        def _():
            for m in range(2):
                to_down(p + s, m).wait_send()


def gather_all(x, model_width, capacity, chosen, devices):
    planes = devices // PLANE
    dma = pltpu.SemaphoreType.DMA
    return pl.pallas_call(
        functools.partial(gather_kernel, planes, capacity, chosen),
        out_shape=(
            jax.ShapeDtypeStruct((PLANE, planes) + x.shape, x.dtype),
            jax.ShapeDtypeStruct((PLANE, planes * 2 * capacity, model_width), x.dtype),
            jax.ShapeDtypeStruct((PLANE, planes) + x.shape[:2] + (128,), x.dtype),
        ),
        in_specs=[pl.BlockSpec(memory_space=pltpu.VMEM)],
        out_specs=(
            pl.BlockSpec(memory_space=pl.ANY),
            pl.BlockSpec(memory_space=pltpu.VMEM),
            pl.BlockSpec(memory_space=pltpu.VMEM),
        ),
        scratch_shapes=[
            pltpu.VMEM((2, planes) + x.shape, x.dtype),
            dma,
            dma((planes, 4, 2)),
            dma((planes, 4)),
            dma((planes, 2)),
            dma((planes, 2)),
            dma((planes, 3)),
            dma((planes, 3)),
            dma((planes, 4)),
            dma((2,)),
        ],
        compiler_params=pltpu.CompilerParams(collective_id=0, has_side_effects=True),
    )(x)


def return_kernel(
    planes, hid_ref, down_ref, matrix_ref, out_ref, w_buf, answers, inbox, sums, column, w_sem, a_send, a_recv, s_send, s_recv
):
    me = lax.axis_index("ep")
    p = me // PLANE
    q = me % PLANE
    chunks, depth, width = w_buf.shape

    def load(c):
        place = pl.multiple_of(c * width, width)
        return pltpu.make_async_copy(
            down_ref.at[:, pl.ds(place, width)], w_buf.at[c], w_sem.at[c]
        )

    for c in range(chunks):
        load(c).start()

    barrier = pltpu.get_barrier_semaphore()
    for i in range(1, PLANE):
        other = p * PLANE + (q + i) % PLANE
        pl.semaphore_signal(barrier, inc=1, device_id=(other,), device_id_type=MESH)
    for i in range(1, planes):
        other = ((p + i) % planes) * PLANE + q
        pl.semaphore_signal(barrier, inc=1, device_id=(other,), device_id_type=MESH)
    pl.semaphore_wait(barrier, PLANE + planes - 2)

    def answer_copy(c, i):
        place = (q + i) % PLANE
        return pltpu.make_async_remote_copy(
            src_ref=answers.at[c, place],
            dst_ref=inbox.at[c, q],
            send_sem=a_send.at[c, i],
            recv_sem=a_recv.at[c, q],
            device_id=(p * PLANE + place,),
            device_id_type=MESH,
        )

    def answer_arrived(c, i):
        place = (q + i) % PLANE
        pltpu.make_async_remote_copy(
            src_ref=answers.at[c, place],
            dst_ref=inbox.at[c, place],
            send_sem=a_send.at[c, i],
            recv_sem=a_recv.at[c, place],
            device_id=(p * PLANE + place,),
            device_id_type=MESH,
        ).wait_recv()

    def sum_copy(c, i):
        place = (p + i) % planes
        return pltpu.make_async_remote_copy(
            src_ref=sums.at[c, place],
            dst_ref=column.at[c, p],
            send_sem=s_send.at[c, i],
            recv_sem=s_recv.at[c, p],
            device_id=(place * PLANE + q,),
            device_id_type=MESH,
        )

    def sum_arrived(c, i):
        place = (p + i) % planes
        pltpu.make_async_remote_copy(
            src_ref=sums.at[c, place],
            dst_ref=column.at[c, place],
            send_sem=s_send.at[c, i],
            recv_sem=s_recv.at[c, place],
            device_id=(place * PLANE + q,),
            device_id_type=MESH,
        ).wait_recv()

    def compute(c, carry):
        load(c).wait()
        found = jnp.dot(hid_ref[...], w_buf[c], preferred_element_type=jnp.float32)
        answers[c] = found.reshape(answers.shape[1:]).astype(jnp.bfloat16)
        for i in range(1, PLANE):
            answer_copy(c, i).start()
        inbox[c, q] = answers[c, q]
        return carry

    lax.fori_loop(0, chunks, compute, 0)

    def combine(c, carry):
        for i in range(1, PLANE):
            answer_arrived(c, i)
        total = jnp.zeros((matrix_ref.shape[2], width), jnp.float32)
        for k in range(PLANE):
            for half in range(2):
                total += jnp.dot(
                    matrix_ref[k, half], inbox[c, k], preferred_element_type=jnp.float32
                )
        sums[c] = total.reshape(sums.shape[1:]).astype(jnp.bfloat16)
        for i in range(1, planes):
            sum_copy(c, i).start()
        column[c, p] = sums[c, p]
        return carry

    lax.fori_loop(0, chunks, combine, 0)

    def gather_sums(c, carry):
        for i in range(1, planes):
            sum_arrived(c, i)
        total = column[c, 0].astype(jnp.float32)
        for k in range(1, planes):
            total += column[c, k].astype(jnp.float32)
        out_ref[c] = total.astype(jnp.bfloat16)
        return carry

    lax.fori_loop(0, chunks, gather_sums, 0)

    def finish(c, carry):
        for i in range(1, PLANE):
            answer_copy(c, i).wait_send()
        for i in range(1, planes):
            sum_copy(c, i).wait_send()
        return carry

    lax.fori_loop(0, chunks, finish, 0)


def return_all(hid, w_down, matrix, devices):
    planes = devices // PLANE
    depth, model_width = w_down.shape
    width = next(w for w in (512, 256, 128) if model_width % w == 0)
    chunks = model_width // width
    rows = hid.shape[0] // PLANE
    tokens = matrix.shape[2] // planes
    dma = pltpu.SemaphoreType.DMA
    vmem = pl.BlockSpec(memory_space=pltpu.VMEM)
    return pl.pallas_call(
        functools.partial(return_kernel, planes),
        out_shape=jax.ShapeDtypeStruct((chunks, tokens, width), jnp.bfloat16),
        in_specs=[vmem, pl.BlockSpec(memory_space=pl.ANY), vmem],
        out_specs=vmem,
        scratch_shapes=[
            pltpu.VMEM((chunks, depth, width), jnp.bfloat16),
            pltpu.VMEM((chunks, PLANE, rows, width), jnp.bfloat16),
            pltpu.VMEM((chunks, PLANE, rows, width), jnp.bfloat16),
            pltpu.VMEM((chunks, planes, tokens, width), jnp.bfloat16),
            pltpu.VMEM((chunks, planes, tokens, width), jnp.bfloat16),
            dma((chunks,)),
            dma((chunks, PLANE)),
            dma((chunks, PLANE)),
            dma((chunks, planes)),
            dma((chunks, planes)),
        ],
        compiler_params=pltpu.CompilerParams(collective_id=1, has_side_effects=True),
    )(hid, w_down, matrix)


def parts_of(values, count):
    parts = []
    for _ in range(count):
        part = lax.reduce_precision(values, 8, 7)
        parts.append(part.astype(jnp.bfloat16))
        values = values - part
    return parts


def ranks(mask):
    rows = mask.shape[-1]
    earlier = (jnp.arange(rows)[:, None] < jnp.arange(rows)[None, :]).astype(jnp.bfloat16)
    found = jnp.einsum(
        "...r,rt->...t", mask.astype(jnp.bfloat16), earlier, preferred_element_type=jnp.float32
    )
    return found.astype(jnp.int32)


def shards(hidden, expert_ids, gate_scores, w_gate, w_up, w_down):
    devices = lax.axis_size("ep")
    planes = devices // PLANE
    me = lax.axis_index("ep")
    my_plane, my_place = me // PLANE, me % PLANE
    micro_count, tok_mb, model_width = hidden.shape
    chosen = expert_ids.shape[2]
    capacity = tok_mb * chosen // devices + 1
    weights = route_scale * gate_scores / jnp.sum(gate_scores, axis=-1, keepdims=True)

    extra = jnp.concatenate([expert_ids.astype(jnp.bfloat16)] + parts_of(weights, 3), axis=-1)
    extra = jnp.pad(extra, ((0, 0), (0, 0), (0, 128 - extra.shape[-1])))
    _, rows, notes = gather_all(
        jnp.concatenate([hidden, extra], axis=-1), model_width, capacity, chosen, devices
    )
    rows = rows.reshape(-1, model_width)
    notes = notes.astype(jnp.float32)
    all_ids = notes[..., :chosen].astype(jnp.int32)
    all_weights = (
        notes[..., chosen : 2 * chosen]
        + notes[..., 2 * chosen : 3 * chosen]
        + notes[..., 3 * chosen : 4 * chosen]
    )
    named = all_ids == me
    expert_load = jnp.sum(jnp.where(named, all_weights, 0.0)).reshape(1) * (
        devices / (route_scale * micro_count * tok_mb * devices)
    )

    slots = jnp.arange(capacity, dtype=jnp.int32)
    gate = jnp.dot(rows, w_gate[0], preferred_element_type=jnp.float32)
    upper = jnp.dot(rows, w_up[0], preferred_element_type=jnp.float32)
    hid = (jax.nn.silu(gate) * upper).astype(jnp.bfloat16)

    ids = lax.dynamic_index_in_dim(all_ids, my_place, 0, keepdims=False)
    share = lax.dynamic_index_in_dim(all_weights, my_place, 0, keepdims=False)
    experts_here = my_plane * PLANE + jnp.arange(PLANE, dtype=jnp.int32)
    same = ids[:, :, None] == experts_here[:, None, None]
    here = jnp.any(same, axis=-1)
    weight_here = jnp.sum(jnp.where(same, share[:, :, None], 0.0), axis=-1)
    spots = here[..., None] & (ranks(here)[..., None] == slots)
    spread = jnp.where(spots, weight_here[..., None], 0.0)
    groups = planes * micro_count
    spread = spread.transpose(2, 0, 1, 3, 4).reshape(PLANE, groups, tok_mb, 1, capacity)
    diag = jnp.eye(groups, dtype=jnp.float32)[:, None, :, None]
    matrix = (spread * diag).reshape(PLANE, groups * tok_mb, groups * capacity)
    matrix = jnp.stack(parts_of(matrix, 2), axis=1)
    mixed = return_all(hid, w_down[0], matrix, devices)
    mixed = mixed.transpose(1, 0, 2)
    return (mixed.reshape(micro_count, tok_mb, model_width), expert_load)


def solution(mesh):
    placed = (
        P(None, "ep", None),
        P(None, "ep", None),
        P(None, "ep", None),
        P("ep", None, None),
        P("ep", None, None),
        P("ep", None, None),
    )
    return jax.shard_map(
        shards,
        mesh=mesh,
        in_specs=placed,
        out_specs=(P(None, "ep", None), P("ep")),
        check_vma=False,
    )
```
